64 devices in a mesh: rep: 8 (over x, y, core), dp: 8 (over z).
Axes of the slice: x: 2, y: 2, z: 8, core: 2. Of those that a mesh axis runs over, the one named last changes fastest.
The devices are a block of a 4x4x8 slice.
Arguments:
- a: bfloat16 [64, 4, 8192, 512], P(('rep', 'dp')), parts along dimension 0
- g: bfloat16 [64, 4, 8192, 1280], P(('rep', 'dp')), parts along dimension 0
Outputs:
- output: bfloat16 [32, 512, 1280], P('rep'), parts along dimension 0
There are 8 independent parts. The reference program is written for one: setup_inputs(seed, part) draws one part's arguments, and reference() takes and returns one part's arrays. A program takes and returns all parts, laid end to end along the dimension named above; each array names one.
All inputs are finite; a program needn't handle non-finite values.
Results may differ from the reference program's by a relative error of at most 0.012.
Values are sent between devices in bfloat16 or wider.
A program may use at most 768 MiB of HBM per device.

```python
import jax
import jax.numpy as jnp
from jax import lax

DEVICES = 8
MATRICES = 4
TOKENS = 8192
D = 512
FF = 1280


def setup_inputs(seed: int = 0, part: int = 0) -> dict:
    ka, kg, ks = (jax.random.fold_in(k, part) for k in jax.random.split(jax.random.key(seed), 3))
    size = 2.0 ** jax.random.uniform(ks, (DEVICES, MATRICES, 1, 1), jnp.float32, -1.0, 1.0)
    a = jax.random.normal(ka, (DEVICES, MATRICES, TOKENS, D), jnp.float32)
    g = size * jax.random.normal(kg, (DEVICES, MATRICES, TOKENS, FF), jnp.float32) * (DEVICES * TOKENS) ** -0.5
    return {"a": a.astype(jnp.bfloat16), "g": g.astype(jnp.bfloat16)}


def reference(a, g):
    def take(so_far, one):
        return so_far + jnp.einsum("ntd,ntf->ndf", *one, preferred_element_type=jnp.float32), None

    return lax.scan(take, jnp.zeros((MATRICES, D, FF), jnp.float32), (a, g))[0].astype(jnp.bfloat16)
```

```python
import functools

import jax
import jax.numpy as jnp
from jax import lax
from jax.experimental import pallas as pl
from jax.experimental.pallas import tpu as pltpu
from jax.sharding import PartitionSpec as P

MESH = pl.DeviceIdType.MESH
COLS = 256
PIECES = 8
DOTS = 4
SLOTS = 6
GBUF = 3


def kernel(shape, a_hbm, g_hbm, out, a_raw, a_t, g_buf, own, first, runs, a_sem, g_sem, send_sem, recv_sem):
    n, matrices, tokens, d, ff = shape
    per = ff // COLS
    chunks = matrices * per
    rows = d // n
    half = rows // 2
    far = n // 2
    me = lax.axis_index("dp")
    right, left = lax.rem(me + 1, n), lax.rem(me + n - 1, n)
    piece = tokens // PIECES
    depth = tokens // DOTS
    low, high = pl.ds(0, half), pl.ds(half, half)

    def owner(offset):
        return lax.rem(me + offset + n, n)

    def rows_of(who, lo=0, size=rows):
        return pl.ds(pl.multiple_of(who * rows + lo, half), size)

    def place(c, who, lo=0, size=rows):
        return out.at[c // per, rows_of(who, lo, size), pl.ds(pl.multiple_of(lax.rem(c, per) * COLS, COLS), COLS)]

    def load_a(m, k):
        r = pl.ds(k * piece, piece)
        return pltpu.make_async_copy(a_hbm.at[0, m, r], a_raw.at[r], a_sem.at[k])

    def load_g(c, k):
        r = pl.ds(k * piece, piece)
        col = pl.ds(pl.multiple_of(lax.rem(c, per) * COLS, COLS), COLS)
        return pltpu.make_async_copy(g_hbm.at[0, c // per, r, col], g_buf.at[lax.rem(c, GBUF), r], g_sem.at[lax.rem(c, GBUF), k])

    def send(way, stage, c, src, dst):
        return pltpu.make_async_remote_copy(
            src_ref=src, dst_ref=dst, send_sem=send_sem.at[way, stage, c], recv_sem=recv_sem.at[way, stage, c],
            device_id={"dp": right if way == 0 else left}, device_id_type=MESH)

    def hop(way, s, c):
        if s == 0:
            part = low if way == 0 else high
            return send(way, 0, c, first.at[c, part], runs.at[way, 0, c, part])
        return send(way, s, c, runs.at[way, s - 1, c], runs.at[way, s, c])

    def originate(c):
        who = owner(far)
        first[c] = own[lax.rem(c, SLOTS), rows_of(who)].astype(jnp.bfloat16)
        for way in (0, 1):
            hop(way, 0, c).start()

    def pass_on(s, c):
        for way in (0, 1):
            who = owner(far - s if way == 0 else s - far)
            hop(way, s - 1, c).wait_recv()
            mine = own.at[lax.rem(c, SLOTS), rows_of(who)]
            if s == 1:
                add, plain = (low, high) if way == 0 else (high, low)
                runs[way, 0, c, add] = (runs[way, 0, c, add].astype(jnp.float32) + mine[add]).astype(jnp.bfloat16)
                runs[way, 0, c, plain] = mine[plain].astype(jnp.bfloat16)
            else:
                runs[way, s - 1, c] = (runs[way, s - 1, c].astype(jnp.float32) + mine[...]).astype(jnp.bfloat16)
            hop(way, s, c).start()

    def spread(way, h, c, who):
        if h == far:
            ref = place(c, who, 0 if way == 0 else half, half)
        else:
            ref = place(c, who)
        return send(way, far + h - 1, c, ref, ref)

    def spread_out(way, h, c):
        return spread(way, h, c, owner(1 - h if way == 0 else h - 1))

    def spread_in(way, h, c):
        return spread(way, h, c, owner(-h if way == 0 else h))

    def finish(c):
        for way in (0, 1):
            hop(way, far - 1, c).wait_recv()
        total = own[lax.rem(c, SLOTS), rows_of(me)]
        total = total + runs[0, far - 1, c].astype(jnp.float32) + runs[1, far - 1, c].astype(jnp.float32)
        place(c, me)[...] = total.astype(jnp.bfloat16)
        for way in (0, 1):
            spread_out(way, 1, c).start()

    def forward(h, c):
        for way in (0, 1):
            spread_in(way, h - 1, c).wait_recv()
            spread_out(way, h, c).start()

    def phase(t, p):
        if p < 3:
            c = t - 2 - p

            @pl.when((c >= 0) & (c < chunks))
            def _():
                pass_on(p + 1, c)
        else:
            @pl.when((t >= 5) & (t < chunks + 5))
            def _():
                finish(t - 5)

            @pl.when(t < chunks)
            def _():
                originate(t)

    def tick(t, m, fresh):
        slot = lax.rem(t, SLOTS)
        buf = lax.rem(t, GBUF)

        @pl.when(t + GBUF - 1 < chunks)
        def _():
            for k in range(PIECES):
                load_g(t + GBUF - 1, k).start()

        if not fresh:
            @pl.when((lax.rem(t, per) == 1) & (m + 1 < matrices))
            def _():
                for k in range(PIECES):
                    load_a(m + 1, k).start()

        for k in range(DOTS):
            for q in range(k * PIECES // DOTS, (k + 1) * PIECES // DOTS):
                if fresh:
                    load_a(m, q).wait()
                load_g(t, q).wait()
            r = pl.ds(k * depth, depth)
            if fresh:
                a_t[:, r] = a_raw[r, :].T
            part = jnp.dot(a_t[:, r], g_buf[buf, r], preferred_element_type=jnp.float32)
            if k == 0:
                own[slot] = part
            else:
                own[slot] += part
            phase(t, k)

    for k in range(PIECES):
        load_a(0, k).start()
        load_g(0, k).start()
    for k in range(PIECES):
        load_g(1, k).start()

    barrier = pltpu.get_barrier_semaphore()
    for other in (left, right):
        pl.semaphore_signal(barrier, inc=1, device_id={"dp": other}, device_id_type=MESH)
    pl.semaphore_wait(barrier, 2)

    @pl.loop(0, matrices)
    def _(m):
        tick(m * per, m, True)

        @pl.loop(1, per)
        def _(j):
            tick(m * per + j, m, False)

    early = 3 * 5

    @pl.loop(0, 5)
    def _(i):
        for p in range(4):
            phase(chunks + i, p)
            if p < 3:
                forward(2, 3 * i + p)

    @pl.loop(early, chunks)
    def _(c):
        forward(2, c)

    for h in range(3, far + 1):
        @pl.loop(0, chunks)
        def _(c):
            forward(h, c)

    @pl.loop(0, chunks)
    def _(c):
        for way in (0, 1):
            spread_in(way, far, c).wait_recv()

    @pl.loop(0, chunks)
    def _(c):
        for way in (0, 1):
            for s in range(far):
                hop(way, s, c).wait_send()
            for h in range(1, far + 1):
                spread_out(way, h, c).wait_send()


def solution(mesh):
    n = mesh.shape["dp"]

    def step(a, g):
        _, matrices, tokens, d = a.shape
        ff = g.shape[-1]
        chunks = matrices * (ff // COLS)
        rows = d // n
        far = n // 2
        bf16, f32 = jnp.bfloat16, jnp.float32
        return pl.pallas_call(
            functools.partial(kernel, (n, matrices, tokens, d, ff)),
            out_shape=jax.ShapeDtypeStruct((matrices, d, ff), bf16),
            in_specs=[pl.BlockSpec(memory_space=pl.ANY)] * 2,
            out_specs=pl.BlockSpec(memory_space=pltpu.VMEM),
            scratch_shapes=[
                pltpu.VMEM((tokens, d), bf16),
                pltpu.VMEM((d, tokens), bf16),
                pltpu.VMEM((GBUF, tokens, COLS), bf16),
                pltpu.VMEM((SLOTS, d, COLS), f32),
                pltpu.VMEM((chunks, rows, COLS), bf16),
                pltpu.VMEM((2, far, chunks, rows, COLS), bf16),
                pltpu.SemaphoreType.DMA((PIECES,)),
                pltpu.SemaphoreType.DMA((GBUF, PIECES)),
                pltpu.SemaphoreType.DMA((2, 2 * far, chunks)),
                pltpu.SemaphoreType.DMA((2, 2 * far, chunks)),
            ],
            compiler_params=pltpu.CompilerParams(
                collective_id=0, has_side_effects=True, vmem_limit_bytes=66_000_000
            ),
        )(a, g)

    return jax.shard_map(
        step, mesh=mesh, in_specs=(P(("rep", "dp")), P(("rep", "dp"))), out_specs=P("rep"), check_vma=False
    )
```

```python
import functools

import jax
import jax.numpy as jnp
from jax import lax
from jax.experimental import pallas as pl
from jax.experimental.pallas import tpu as pltpu
from jax.sharding import PartitionSpec as P

MESH = pl.DeviceIdType.MESH
COLS = 256
PIECES = 8
DOTS = 2
LAG = 5
SLOTS = LAG + 1
GBUF = 3


def when(condition, then):
    if isinstance(condition, bool):
        if condition:
            then()
    else:
        pl.when(condition)(then)


def kernel(shape, a_hbm, g_hbm, out, a_raw, a_t, g_buf, own, first, runs, a_sem, g_sem, send_sem, recv_sem):
    n, matrices, tokens, d, ff = shape
    per = ff // COLS
    chunks = matrices * per
    rows = d // n
    half = rows // 2
    far = n // 2
    me = lax.axis_index("dp")
    right, left = lax.rem(me + 1, n), lax.rem(me + n - 1, n)
    piece = tokens // PIECES
    low, high = pl.ds(0, half), pl.ds(half, half)

    def owner(offset):
        return lax.rem(me + offset + n, n)

    def rows_of(who, lo=0, size=rows):
        return pl.ds(pl.multiple_of(who * rows + lo, half), size)

    def place(c, who, lo=0, size=rows):
        return out.at[c // per, rows_of(who, lo, size), pl.ds(pl.multiple_of(lax.rem(c, per) * COLS, COLS), COLS)]

    def load_a(m, k):
        r = pl.ds(k * piece, piece)
        return pltpu.make_async_copy(a_hbm.at[0, m, r], a_raw.at[r], a_sem.at[k])

    def load_g(c, k):
        r = pl.ds(k * piece, piece)
        col = pl.ds(pl.multiple_of(lax.rem(c, per) * COLS, COLS), COLS)
        return pltpu.make_async_copy(g_hbm.at[0, c // per, r, col], g_buf.at[lax.rem(c, GBUF), r], g_sem.at[lax.rem(c, GBUF), k])

    def send(way, stage, c, src, dst):
        return pltpu.make_async_remote_copy(
            src_ref=src, dst_ref=dst, send_sem=send_sem.at[way, stage, c], recv_sem=recv_sem.at[way, stage, c],
            device_id={"dp": right if way == 0 else left}, device_id_type=MESH)

    def hop(way, s, c):
        if s == 0:
            part = low if way == 0 else high
            return send(way, 0, c, first.at[c, part], runs.at[way, 0, c, part])
        return send(way, s, c, runs.at[way, s - 1, c], runs.at[way, s, c])

    def originate(c):
        who = owner(far)
        first[c] = own[lax.rem(c, SLOTS), rows_of(who)].astype(jnp.bfloat16)
        for way in (0, 1):
            hop(way, 0, c).start()

    def pass_on(s, c):
        for way in (0, 1):
            who = owner(far - s if way == 0 else s - far)
            hop(way, s - 1, c).wait_recv()
            mine = own.at[lax.rem(c, SLOTS), rows_of(who)]
            if s == 1:
                add, plain = (low, high) if way == 0 else (high, low)
                runs[way, 0, c, add] = (runs[way, 0, c, add].astype(jnp.float32) + mine[add]).astype(jnp.bfloat16)
                runs[way, 0, c, plain] = mine[plain].astype(jnp.bfloat16)
            else:
                runs[way, s - 1, c] = (runs[way, s - 1, c].astype(jnp.float32) + mine[...]).astype(jnp.bfloat16)
            hop(way, s, c).start()

    def spread(way, h, c, who):
        if h == 1:
            ref = place(c, who)
        elif h == far:
            ref = out.at[c, rows_of(who, 0 if way == 0 else half, half)]
        else:
            ref = out.at[c, rows_of(who)]
        return send(way, far + h - 1, c, ref, ref)

    def spread_out(way, h, c):
        return spread(way, h, c, owner(1 - h if way == 0 else h - 1))

    def spread_in(way, h, c):
        return spread(way, h, c, owner(-h if way == 0 else h))

    def finish(c):
        for way in (0, 1):
            hop(way, far - 1, c).wait_recv()
        total = own[lax.rem(c, SLOTS), rows_of(me)]
        total = total + runs[0, far - 1, c].astype(jnp.float32) + runs[1, far - 1, c].astype(jnp.float32)
        place(c, me)[...] = total.astype(jnp.bfloat16)
        for way in (0, 1):
            spread_out(way, 1, c).start()

    def forward(h, m):
        for way in (0, 1):
            if h == 2:
                for j in range(per):
                    spread_in(way, 1, m * per + j).wait_recv()
            else:
                spread_in(way, h - 1, m).wait_recv()
            spread_out(way, h, m).start()

    def phase(t, p):
        def hops(s, c):
            when((c >= 0) & (c < chunks), lambda: pass_on(s, c))

        if p == 0:
            hops(2, t - 3)
            hops(3, t - 4)
        else:
            when(t < chunks, lambda: originate(t))
            hops(1, t - 1)
            when((t >= LAG) & (t < chunks + LAG), lambda: finish(t - LAG))

    def tick(t, m, fresh, dots=DOTS):
        slot = lax.rem(t, SLOTS)
        buf = lax.rem(t, GBUF)

        def more():
            for k in range(PIECES):
                load_g(t + GBUF - 1, k).start()

        if dots == DOTS:
            when(t + GBUF - 1 < chunks, more)

        if not fresh:
            @pl.when((lax.rem(t, per) == 1) & (m + 1 < matrices))
            def _():
                for k in range(PIECES):
                    load_a(m + 1, k).start()

        depth = tokens // dots
        for k in range(dots):
            for q in range(k * PIECES // dots, (k + 1) * PIECES // dots):
                if fresh:
                    load_a(m, q).wait()
                load_g(t, q).wait()
            if dots == PIECES and k >= 5:
                for q in ((0, 1), (2, 3, 4), (5, 6, 7))[k - 5]:
                    load_g(1, q).start()
            r = pl.ds(k * depth, depth)
            if fresh:
                a_t[:, r] = a_raw[r, :].T
            for i in range(2):
                rr = pl.ds(i * (d // 2), d // 2)
                part = jnp.dot(a_t[rr, r], g_buf[buf, r], preferred_element_type=jnp.float32)
                if k == 0:
                    own[slot, rr] = part
                else:
                    own[slot, rr] += part
            if dots == DOTS:
                phase(t, k)

    barrier = pltpu.get_barrier_semaphore()
    for other in (left, right):
        pl.semaphore_signal(barrier, inc=1, device_id={"dp": other}, device_id_type=MESH)

    for k in range(PIECES):
        load_a(0, k).start()
        load_g(0, k).start()

    tick(0, 0, True, PIECES)
    pl.semaphore_wait(barrier, 2)
    originate(0)
    for k in range(PIECES):
        load_g(2, k).start()

    @pl.loop(1, per)
    def _(t):
        tick(t, 0, False)

    @pl.loop(1, matrices)
    def _(m):
        tick(m * per, m, True)

        @pl.loop(1, per)
        def _(j):
            tick(m * per + j, m, False)

    for i in range(LAG):
        for p in range(DOTS):
            phase(chunks + i, p)
        if i in (0, 2):
            forward(2, i // 2)

    for h, m in ((2, 2), (3, 0), (2, 3), (3, 1), (4, 0), (3, 2), (4, 1), (3, 3), (4, 2), (4, 3)):
        forward(h, m)

    for m in range(matrices):
        for way in (0, 1):
            spread_in(way, far, m).wait_recv()

    @pl.loop(0, chunks)
    def _(c):
        for way in (0, 1):
            for s in range(far):
                hop(way, s, c).wait_send()
            spread_out(way, 1, c).wait_send()

    for m in range(matrices):
        for way in (0, 1):
            for h in range(2, far + 1):
                spread_out(way, h, m).wait_send()


def solution(mesh):
    n = mesh.shape["dp"]

    def step(a, g):
        _, matrices, tokens, d = a.shape
        ff = g.shape[-1]
        chunks = matrices * (ff // COLS)
        rows = d // n
        far = n // 2
        bf16, f32 = jnp.bfloat16, jnp.float32
        return pl.pallas_call(
            functools.partial(kernel, (n, matrices, tokens, d, ff)),
            out_shape=pltpu.VMEM((matrices, d, ff), bf16),
            in_specs=[pl.BlockSpec(memory_space=pl.ANY)] * 2,
            out_specs=pl.BlockSpec(memory_space=pltpu.VMEM),
            scratch_shapes=[
                pltpu.VMEM((tokens, d), bf16),
                pltpu.VMEM((d, tokens), bf16),
                pltpu.VMEM((GBUF, tokens, COLS), bf16),
                pltpu.VMEM((SLOTS, d, COLS), f32),
                pltpu.VMEM((chunks, rows, COLS), bf16),
                pltpu.VMEM((2, far, chunks, rows, COLS), bf16),
                pltpu.SemaphoreType.DMA((PIECES,)),
                pltpu.SemaphoreType.DMA((GBUF, PIECES)),
                pltpu.SemaphoreType.DMA((2, 2 * far, chunks)),
                pltpu.SemaphoreType.DMA((2, 2 * far, chunks)),
            ],
            compiler_params=pltpu.CompilerParams(
                collective_id=0, has_side_effects=True, vmem_limit_bytes=56_000_000
            ),
        )(a, g)

    return jax.shard_map(
        step, mesh=mesh, in_specs=(P(("rep", "dp")), P(("rep", "dp"))), out_specs=P("rep"), check_vma=False
    )
```

```python
import functools

import jax
import jax.numpy as jnp
from jax import lax
from jax.experimental import pallas as pl
from jax.experimental.pallas import tpu as pltpu
from jax.sharding import PartitionSpec as P

MESH = pl.DeviceIdType.MESH
COLS = 256
PIECES = 8
DOTS = 2
LAG = 5
SLOTS = LAG + 1
GBUF = 3


def when(condition, then):
    if isinstance(condition, bool):
        if condition:
            then()
    else:
        pl.when(condition)(then)


def kernel(shape, a_hbm, g_hbm, out, a_raw, a_t, g_buf, own, first, runs, a_sem, g_sem, send_sem, recv_sem):
    n, matrices, tokens, d, ff = shape
    per = ff // COLS
    chunks = matrices * per
    rows = d // n
    half = rows // 2
    far = n // 2
    me = lax.axis_index("dp")
    right, left = lax.rem(me + 1, n), lax.rem(me + n - 1, n)
    piece = tokens // PIECES
    low, high = pl.ds(0, half), pl.ds(half, half)

    def owner(offset):
        return lax.rem(me + offset + n, n)

    def rows_of(who, lo=0, size=rows):
        return pl.ds(pl.multiple_of(who * rows + lo, half), size)

    def place(c, who, lo=0, size=rows):
        return out.at[c // per, rows_of(who, lo, size), pl.ds(pl.multiple_of(lax.rem(c, per) * COLS, COLS), COLS)]

    def load_a(m, k):
        r = pl.ds(k * piece, piece)
        return pltpu.make_async_copy(a_hbm.at[0, m, r], a_raw.at[r], a_sem.at[k])

    def load_g(c, k):
        r = pl.ds(k * piece, piece)
        col = pl.ds(pl.multiple_of(lax.rem(c, per) * COLS, COLS), COLS)
        return pltpu.make_async_copy(g_hbm.at[0, c // per, r, col], g_buf.at[lax.rem(c, GBUF), r], g_sem.at[lax.rem(c, GBUF), k])

    def send(way, stage, c, src, dst):
        return pltpu.make_async_remote_copy(
            src_ref=src, dst_ref=dst, send_sem=send_sem.at[way, stage, c], recv_sem=recv_sem.at[way, stage, c],
            device_id={"dp": right if way == 0 else left}, device_id_type=MESH)

    def hop(way, s, c):
        if s == 0:
            part = low if way == 0 else high
            return send(way, 0, c, first.at[c, part], runs.at[way, 0, c, part])
        return send(way, s, c, runs.at[way, s - 1, c], runs.at[way, s, c])

    def originate(c):
        who = owner(far)
        first[c] = own[lax.rem(c, SLOTS), rows_of(who)].astype(jnp.bfloat16)
        for way in (0, 1):
            hop(way, 0, c).start()

    def pass_on(s, c):
        for way in (0, 1):
            who = owner(far - s if way == 0 else s - far)
            hop(way, s - 1, c).wait_recv()
            mine = own.at[lax.rem(c, SLOTS), rows_of(who)]
            if s == 1:
                add, plain = (low, high) if way == 0 else (high, low)
                runs[way, 0, c, add] = (runs[way, 0, c, add].astype(jnp.float32) + mine[add]).astype(jnp.bfloat16)
                runs[way, 0, c, plain] = mine[plain].astype(jnp.bfloat16)
            else:
                runs[way, s - 1, c] = (runs[way, s - 1, c].astype(jnp.float32) + mine[...]).astype(jnp.bfloat16)
            hop(way, s, c).start()

    def spread(way, h, c, who):
        if h == 1:
            ref = place(c, who)
        elif h == far:
            ref = out.at[c, rows_of(who, 0 if way == 0 else half, half)]
        else:
            ref = out.at[c, rows_of(who)]
        return send(way, far + h - 1, c, ref, ref)

    def spread_out(way, h, c):
        return spread(way, h, c, owner(1 - h if way == 0 else h - 1))

    def spread_in(way, h, c):
        return spread(way, h, c, owner(-h if way == 0 else h))

    def finish(c):
        for way in (0, 1):
            hop(way, far - 1, c).wait_recv()
        total = own[lax.rem(c, SLOTS), rows_of(me)]
        total = total + runs[0, far - 1, c].astype(jnp.float32) + runs[1, far - 1, c].astype(jnp.float32)
        place(c, me)[...] = total.astype(jnp.bfloat16)
        for way in (0, 1):
            spread_out(way, 1, c).start()

    def forward(h, m):
        for way in (0, 1):
            if h == 2:
                for j in range(per):
                    spread_in(way, 1, m * per + j).wait_recv()
            else:
                spread_in(way, h - 1, m).wait_recv()
            spread_out(way, h, m).start()

    def phase(t, p):
        def hops(s, c):
            when((c >= 0) & (c < chunks), lambda: pass_on(s, c))

        if p == 0:
            hops(2, t - 3)
            hops(3, t - 4)
        else:
            when(t < chunks, lambda: originate(t))
            hops(1, t - 1)
            when((t >= LAG) & (t < chunks + LAG), lambda: finish(t - LAG))

    def tick(t, m, fresh, dots=DOTS):
        slot = lax.rem(t, SLOTS)
        buf = lax.rem(t, GBUF)

        def more():
            for k in range(PIECES):
                load_g(t + GBUF - 1, k).start()

        if dots == DOTS:
            when(t + GBUF - 1 < chunks, more)

        if not fresh:
            @pl.when((lax.rem(t, per) == 1) & (m + 1 < matrices))
            def _():
                for k in range(PIECES):
                    load_a(m + 1, k).start()

        depth = tokens // dots
        for k in range(dots):
            for q in range(k * PIECES // dots, (k + 1) * PIECES // dots):
                if fresh:
                    load_a(m, q).wait()
                load_g(t, q).wait()
            if dots == PIECES and k >= 5:
                for q in ((0, 1), (2, 3, 4), (5, 6, 7))[k - 5]:
                    load_g(1, q).start()
            r = pl.ds(k * depth, depth)
            if fresh:
                a_t[:, r] = a_raw[r, :].T
            for i in range(2):
                rr = pl.ds(i * (d // 2), d // 2)
                part = jnp.dot(a_t[rr, r], g_buf[buf, r], preferred_element_type=jnp.float32)
                if k == 0:
                    own[slot, rr] = part
                else:
                    own[slot, rr] += part
            if dots == DOTS:
                phase(t, k)

    barrier = pltpu.get_barrier_semaphore()
    for other in (left, right):
        pl.semaphore_signal(barrier, inc=1, device_id={"dp": other}, device_id_type=MESH)

    for k in range(PIECES):
        load_a(0, k).start()
        load_g(0, k).start()

    tick(0, 0, True, PIECES)
    pl.semaphore_wait(barrier, 2)
    originate(0)
    for k in range(PIECES):
        load_g(2, k).start()

    @pl.loop(1, per)
    def _(t):
        tick(t, 0, False)

    @pl.loop(1, matrices)
    def _(m):
        tick(m * per, m, True)

        @pl.loop(1, per)
        def _(j):
            tick(m * per + j, m, False)

    between = ((2, 0), (2, 1), (2, 2), (3, 0), (3, 1))
    for i in range(LAG):
        for p in range(DOTS):
            phase(chunks + i, p)
        forward(*between[i])

    forward(2, 3)
    forward(3, 2)

    @pl.loop(0, chunks)
    def _(c):
        for way in (0, 1):
            for s in range(far):
                hop(way, s, c).wait_send()
            spread_out(way, 1, c).wait_send()

    for h, m in ((3, 3), (4, 0), (4, 1), (4, 2), (4, 3)):
        forward(h, m)

    for h in range(2, far):
        for m in range(matrices):
            for way in (0, 1):
                spread_out(way, h, m).wait_send()

    for m in range(matrices):
        for way in (0, 1):
            spread_out(way, far, m).wait_send()
            spread_in(way, far, m).wait_recv()


def solution(mesh):
    n = mesh.shape["dp"]

    def step(a, g):
        _, matrices, tokens, d = a.shape
        ff = g.shape[-1]
        chunks = matrices * (ff // COLS)
        rows = d // n
        far = n // 2
        bf16, f32 = jnp.bfloat16, jnp.float32
        return pl.pallas_call(
            functools.partial(kernel, (n, matrices, tokens, d, ff)),
            out_shape=pltpu.VMEM((matrices, d, ff), bf16),
            in_specs=[pl.BlockSpec(memory_space=pl.ANY)] * 2,
            out_specs=pl.BlockSpec(memory_space=pltpu.VMEM),
            scratch_shapes=[
                pltpu.VMEM((tokens, d), bf16),
                pltpu.VMEM((d, tokens), bf16),
                pltpu.VMEM((GBUF, tokens, COLS), bf16),
                pltpu.VMEM((SLOTS, d, COLS), f32),
                pltpu.VMEM((chunks, rows, COLS), bf16),
                pltpu.VMEM((2, far, chunks, rows, COLS), bf16),
                pltpu.SemaphoreType.DMA((PIECES,)),
                pltpu.SemaphoreType.DMA((GBUF, PIECES)),
                pltpu.SemaphoreType.DMA((2, 2 * far, chunks)),
                pltpu.SemaphoreType.DMA((2, 2 * far, chunks)),
            ],
            compiler_params=pltpu.CompilerParams(
                collective_id=0, has_side_effects=True, vmem_limit_bytes=56_000_000
            ),
        )(a, g)

    return jax.shard_map(
        step, mesh=mesh, in_specs=(P(("rep", "dp")), P(("rep", "dp"))), out_specs=P("rep"), check_vma=False
    )
```

```python
import functools

import jax
import jax.numpy as jnp
from jax import lax
from jax.experimental import pallas as pl
from jax.experimental.pallas import tpu as pltpu
from jax.sharding import PartitionSpec as P

MESH = pl.DeviceIdType.MESH
COLS = 256
PIECES = 8
DOTS = 2
LAG = 6
SLOTS = LAG + 1
GBUF = 3


def when(condition, then):
    if isinstance(condition, bool):
        if condition:
            then()
    else:
        pl.when(condition)(then)


def kernel(shape, a_hbm, g_hbm, out, a_raw, a_t, g_buf, own, first, runs, a_sem, g_sem, send_sem, recv_sem):
    n, matrices, tokens, d, ff = shape
    per = ff // COLS
    chunks = matrices * per
    rows = d // n
    half = rows // 2
    far = n // 2
    me = lax.axis_index("dp")
    right, left = lax.rem(me + 1, n), lax.rem(me + n - 1, n)
    piece = tokens // PIECES
    low, high = pl.ds(0, half), pl.ds(half, half)

    def owner(offset):
        return lax.rem(me + offset + n, n)

    def rows_of(who, lo=0, size=rows):
        return pl.ds(pl.multiple_of(who * rows + lo, half), size)

    def place(c, who, lo=0, size=rows):
        return out.at[c // per, rows_of(who, lo, size), pl.ds(pl.multiple_of(lax.rem(c, per) * COLS, COLS), COLS)]

    def load_a(m, k):
        r = pl.ds(k * piece, piece)
        return pltpu.make_async_copy(a_hbm.at[0, m, r], a_raw.at[r], a_sem.at[k])

    def load_g(c, k):
        r = pl.ds(k * piece, piece)
        col = pl.ds(pl.multiple_of(lax.rem(c, per) * COLS, COLS), COLS)
        return pltpu.make_async_copy(g_hbm.at[0, c // per, r, col], g_buf.at[lax.rem(c, GBUF), r], g_sem.at[lax.rem(c, GBUF), k])

    def send(way, stage, c, src, dst):
        return pltpu.make_async_remote_copy(
            src_ref=src, dst_ref=dst, send_sem=send_sem.at[way, stage, c], recv_sem=recv_sem.at[way, stage, c],
            device_id={"dp": right if way == 0 else left}, device_id_type=MESH)

    def long_of(way):
        return low if way == 0 else high

    def short_of(way):
        return high if way == 0 else low

    def hop(way, s, c):
        src = first.at[way, c] if s == 0 else runs.at[way, s - 1, c]
        dst = runs.at[way, s, c]
        if s == far - 1:
            src, dst = src.at[long_of(way)], dst.at[long_of(way)]
        return send(way, s, c, src, dst)

    def mine(way, s, c, part):
        hops = far - s if part is long_of(way) else far - 1 - s
        return own[lax.rem(c, SLOTS), rows_of(owner(hops if way == 0 else -hops), part.start, half)]

    def originate(c):
        for way in (0, 1):
            for part in (low, high):
                first[way, c, part] = mine(way, 0, c, part).astype(jnp.bfloat16)
            hop(way, 0, c).start()

    def pass_on(s, c):
        for way in (0, 1):
            hop(way, s - 1, c).wait_recv()
            for part in (low, high) if s < far - 1 else (long_of(way),):
                total = runs[way, s - 1, c, part].astype(jnp.float32) + mine(way, s, c, part)
                runs[way, s - 1, c, part] = total.astype(jnp.bfloat16)
            hop(way, s, c).start()

    def spread(way, h, c, who):
        if h == 1:
            ref = place(c, who)
        elif h == far:
            ref = out.at[c, rows_of(who, 0 if way == 0 else half, half)]
        else:
            ref = out.at[c, rows_of(who)]
        return send(way, far + h - 1, c, ref, ref)

    def spread_out(way, h, c):
        return spread(way, h, c, owner(1 - h if way == 0 else h - 1))

    def spread_in(way, h, c):
        return spread(way, h, c, owner(-h if way == 0 else h))

    def finish(c):
        for way in (0, 1):
            hop(way, far - 1, c).wait_recv()
        for way in (0, 1):
            part = long_of(way)
            total = own[lax.rem(c, SLOTS), rows_of(me, part.start, half)]
            total = total + runs[way, far - 1, c, part].astype(jnp.float32) + runs[1 - way, far - 2, c, part].astype(jnp.float32)
            place(c, me, part.start, half)[...] = total.astype(jnp.bfloat16)
        for way in (0, 1):
            spread_out(way, 1, c).start()

    def forward(h, m):
        for way in (0, 1):
            if h == 2:
                for j in range(per):
                    spread_in(way, 1, m * per + j).wait_recv()
            else:
                spread_in(way, h - 1, m).wait_recv()
            spread_out(way, h, m).start()

    def phase(t, p):
        def hops(s, c):
            when((c >= 0) & (c < chunks), lambda: pass_on(s, c))

        if p == 0:
            hops(1, t - 2)
            hops(3, t - 5)
        else:
            when(t < chunks, lambda: originate(t))
            hops(2, t - 3)
            when((t >= LAG) & (t < chunks + LAG), lambda: finish(t - LAG))

    def tick(t, m, fresh, dots=DOTS):
        slot = lax.rem(t, SLOTS)
        buf = lax.rem(t, GBUF)

        def more():
            for k in range(PIECES):
                load_g(t + GBUF - 1, k).start()

        if dots == DOTS:
            when(t + GBUF - 1 < chunks, more)

        if not fresh:
            @pl.when((lax.rem(t, per) == 1) & (m + 1 < matrices))
            def _():
                for k in range(PIECES):
                    load_a(m + 1, k).start()

        depth = tokens // dots
        for k in range(dots):
            for q in range(k * PIECES // dots, (k + 1) * PIECES // dots):
                if fresh:
                    load_a(m, q).wait()
                load_g(t, q).wait()
            if dots == PIECES and k >= 5:
                for q in ((0, 1), (2, 3, 4), (5, 6, 7))[k - 5]:
                    load_g(1, q).start()
            r = pl.ds(k * depth, depth)
            if fresh:
                a_t[:, r] = a_raw[r, :].T
            for i in range(2):
                rr = pl.ds(i * (d // 2), d // 2)
                part = jnp.dot(a_t[rr, r], g_buf[buf, r], preferred_element_type=jnp.float32)
                if k == 0:
                    own[slot, rr] = part
                else:
                    own[slot, rr] += part
            if dots == DOTS:
                phase(t, k)

    barrier = pltpu.get_barrier_semaphore()
    for other in (left, right):
        pl.semaphore_signal(barrier, inc=1, device_id={"dp": other}, device_id_type=MESH)

    for k in range(PIECES):
        load_a(0, k).start()
        load_g(0, k).start()

    tick(0, 0, True, PIECES)
    pl.semaphore_wait(barrier, 2)
    originate(0)
    for k in range(PIECES):
        load_g(2, k).start()

    @pl.loop(1, per)
    def _(t):
        tick(t, 0, False)

    @pl.loop(1, matrices)
    def _(m):
        tick(m * per, m, True)

        @pl.loop(1, per)
        def _(j):
            tick(m * per + j, m, False)

    between = ((2, 0), (2, 1), (2, 2), (3, 0), (3, 1))
    for i in range(LAG):
        for p in range(DOTS):
            phase(chunks + i, p)
        if i > 0:
            forward(*between[i - 1])

    forward(2, 3)
    forward(3, 2)

    @pl.loop(0, chunks)
    def _(c):
        for way in (0, 1):
            for s in range(far):
                hop(way, s, c).wait_send()
            spread_out(way, 1, c).wait_send()

    for h, m in ((3, 3), (4, 0), (4, 1), (4, 2), (4, 3)):
        forward(h, m)

    for h in range(2, far):
        for m in range(matrices):
            for way in (0, 1):
                spread_out(way, h, m).wait_send()

    for m in range(matrices):
        for way in (0, 1):
            spread_out(way, far, m).wait_send()
            spread_in(way, far, m).wait_recv()


def solution(mesh):
    n = mesh.shape["dp"]

    def step(a, g):
        _, matrices, tokens, d = a.shape
        ff = g.shape[-1]
        chunks = matrices * (ff // COLS)
        rows = d // n
        far = n // 2
        bf16, f32 = jnp.bfloat16, jnp.float32
        return pl.pallas_call(
            functools.partial(kernel, (n, matrices, tokens, d, ff)),
            out_shape=pltpu.VMEM((matrices, d, ff), bf16),
            in_specs=[pl.BlockSpec(memory_space=pl.ANY)] * 2,
            out_specs=pl.BlockSpec(memory_space=pltpu.VMEM),
            scratch_shapes=[
                pltpu.VMEM((tokens, d), bf16),
                pltpu.VMEM((d, tokens), bf16),
                pltpu.VMEM((GBUF, tokens, COLS), bf16),
                pltpu.VMEM((SLOTS, d, COLS), f32),
                pltpu.VMEM((2, chunks, rows, COLS), bf16),
                pltpu.VMEM((2, far, chunks, rows, COLS), bf16),
                pltpu.SemaphoreType.DMA((PIECES,)),
                pltpu.SemaphoreType.DMA((GBUF, PIECES)),
                pltpu.SemaphoreType.DMA((2, 2 * far, chunks)),
                pltpu.SemaphoreType.DMA((2, 2 * far, chunks)),
            ],
            compiler_params=pltpu.CompilerParams(
                collective_id=0, has_side_effects=True, vmem_limit_bytes=56_000_000
            ),
        )(a, g)

    return jax.shard_map(
        step, mesh=mesh, in_specs=(P(("rep", "dp")), P(("rep", "dp"))), out_specs=P("rep"), check_vma=False
    )
```
